8 devices in a mesh: dp: 8 (over z, y, x, core).
Axes of the slice: x: 2, y: 2, z: 1, core: 2. Of those that a mesh axis runs over, the one named last changes fastest.
Arguments:
- hidden: bfloat16 [32768, 4096], P('dp')
- router_w: bfloat16 [4096, 128], replicated
- expert_idx: int32 [32768, 8], P('dp')
- gate_grad: float32 [32768, 8], P('dp')
Outputs:
- output 1: float32 [32768, 8], P('dp')
- output 2: float32 [], replicated
- output 3: bfloat16 [32768, 4096], P('dp')
- output 4: float32 [4096, 128], replicated
All inputs are finite; a program needn't handle non-finite values.
Results may differ from the reference program's by a relative error of at most 0.00790332.
Values sent between devices are 32-bit elements.
A program may use at most 1 GiB of HBM per device.

```python
import jax
import jax.numpy as jnp
from jax import lax

TOKENS = 32768
HIDDEN = 4096
EXPERTS = 128
TOP_K = 8
SHARDS = 8
ALPHA = 0.001
ROWS_PER_SHARD = TOKENS // SHARDS
LOSS_SCALE = float(TOKENS * EXPERTS * EXPERTS)


def draw_routes(key):
    key_bias, key_noise, key_shift = jax.random.split(key, 3)
    shard_bias = jax.random.randint(key_bias, (SHARDS, EXPERTS), 0, 48)
    row_noise = jax.random.randint(key_noise, (TOKENS, EXPERTS), 0, 32)
    row_shift = jax.random.randint(key_shift, (SHARDS, 1), 0, EXPERTS)
    row_pos = jnp.arange(ROWS_PER_SHARD)[None, :] + row_shift
    forced = (row_pos % EXPERTS).reshape(TOKENS, 1)
    expert_ids = jnp.arange(EXPERTS)[None, :]
    scores = jnp.repeat(shard_bias, ROWS_PER_SHARD, axis=0) + row_noise + 1000 * (expert_ids == forced).astype(jnp.int32)
    scores = scores * EXPERTS + expert_ids
    chosen = lax.top_k(scores, TOP_K)[1]
    return chosen.astype(jnp.int32)


def setup_inputs(seed: int = 0) -> dict:
    keys = jax.random.split(jax.random.key(seed), 5)
    shard_mean = 0.5 * jax.random.normal(keys[0], (SHARDS, HIDDEN), jnp.float32)
    hidden = jax.random.normal(keys[1], (TOKENS, HIDDEN), jnp.float32) + jnp.repeat(shard_mean, ROWS_PER_SHARD, axis=0)
    router_w = jax.random.normal(keys[2], (HIDDEN, EXPERTS), jnp.float32) * HIDDEN ** -0.5
    expert_idx = draw_routes(keys[3])
    grad_scale = ALPHA * TOP_K * TOP_K / (TOKENS * EXPERTS)
    gate_grad = jax.random.normal(keys[4], (TOKENS, TOP_K), jnp.float32) * grad_scale
    return {"hidden": hidden.astype(jnp.bfloat16), "router_w": router_w.astype(jnp.bfloat16), "expert_idx": expert_idx, "gate_grad": gate_grad}


def reference(hidden, router_w, expert_idx, gate_grad):
    logits = jnp.dot(hidden, router_w, preferred_element_type=jnp.float32)
    expert_freq = jnp.bincount(expert_idx.reshape(-1), length=EXPERTS).astype(jnp.float32) / TOKENS

    def objective(logit_vals):
        router_probs = jax.nn.softmax(logit_vals, axis=-1)
        picked = jnp.take_along_axis(router_probs, expert_idx, axis=1)
        gate_probs = picked / jnp.sum(picked, axis=1, keepdims=True)
        aux_loss = ALPHA * EXPERTS * jnp.sum(expert_freq * jnp.mean(router_probs, axis=0))
        return gate_probs, aux_loss

    (gate_probs, aux_loss), pullback = jax.vjp(objective, logits)
    logit_grad = pullback((LOSS_SCALE * gate_grad, jnp.asarray(LOSS_SCALE, jnp.float32)))[0]
    grad_bf = logit_grad.astype(jnp.bfloat16)
    hidden_grad = jnp.dot(grad_bf, router_w.T, preferred_element_type=jnp.float32).astype(jnp.bfloat16)
    router_grad = jnp.dot(hidden.T, grad_bf, preferred_element_type=jnp.float32)
    return gate_probs, aux_loss, hidden_grad, router_grad
```

```python
import jax
import jax.numpy as jnp
from jax import lax
from jax.experimental import pallas as pl
from jax.experimental.pallas import tpu as pltpu
from jax.sharding import PartitionSpec as P

LOSS_ALPHA = 0.001
MESH = pl.DeviceIdType.MESH
LANES = 128


def neighbours():
    me = lax.axis_index("dp")
    core, x, y = me % 2, (me // 2) % 2, me // 4
    def at(flip):
        fy, fx, fc = (flip // 4) % 2, (flip // 2) % 2, flip % 2
        return (1 - y if fy else y) * 4 + (1 - x if fx else x) * 2 + (1 - core if fc else core)
    return me, at


def remote(src, dst, send_sem, recv_sem, device):
    return pltpu.make_async_remote_copy(src_ref=src, dst_ref=dst, send_sem=send_sem, recv_sem=recv_sem, device_id=(device,), device_id_type=MESH)


def router_kernel(total_rows, hidden_hbm, w_hbm, idx_hbm, gg_hbm, gate_ref, aux_ref, gt_ref, rg_hbm,
                  hid, w, idx, gg, logit_t, count_acc, prob_acc, f_bcast, cnt, prob, send_part, own, from_part, from_x, from_y, gather,
                  load_sem, small_sem, cnt_send, cnt_recv, prob_send, prob_recv, part_send, part_recv, x_send, x_recv, y_send, y_recv,
                  gat_send, gat_recv, out_sem):
    rows, width = hid.shape
    experts, top_k = w.shape[1], idx.shape[0]
    shard = width // 8
    half = experts // 2
    block = 256
    blocks = rows // block
    me, at = neighbours()
    core = me % 2
    chip = me // 2
    loss_scale = float(total_rows * experts * experts)
    aux_coef = loss_scale * LOSS_ALPHA * experts / total_rows

    small = [pltpu.make_async_copy(idx_hbm, idx, small_sem.at[0]), pltpu.make_async_copy(w_hbm, w, small_sem.at[1]), pltpu.make_async_copy(gg_hbm, gg, small_sem.at[2])]
    for c in small:
        c.start()

    def load(b):
        part = pl.ds(b * block, block)
        return pltpu.make_async_copy(hidden_hbm.at[part], hid.at[part], load_sem.at[b])

    for b in range(blocks):
        load(b).start()

    barrier = pltpu.get_barrier_semaphore()
    for k in range(1, 8):
        pl.semaphore_signal(barrier, inc=1, device_id=(at(k),), device_id_type=MESH)

    expert_id = lax.broadcasted_iota(jnp.int32, (experts, LANES), 0)

    def hits(t):
        ids = idx[:, pl.ds(t * LANES, LANES)]
        return [expert_id == ids[j:j + 1, :] for j in range(top_k)]

    def count_tile(t):
        total = count_acc[...]
        for hit in hits(t):
            total = total + jnp.where(hit, 1.0, 0.0)
        count_acc[...] = total

    def logits(b):
        load(b).wait()
        part = pl.ds(b * block, block)
        out = jnp.dot(hid[part, :], w[...], preferred_element_type=jnp.float32)
        logit_t[:, part] = out.T

    def backward_tile(t):
        part = pl.ds(t * LANES, LANES)
        hit = hits(t)
        val = logit_t[:, part]
        val = jnp.exp(val - jnp.max(val, axis=0, keepdims=True))
        p = val * (1.0 / jnp.sum(val, axis=0, keepdims=True))
        prob_acc[...] += p
        picked = jnp.concatenate([jnp.sum(jnp.where(h, p, 0.0), axis=0, keepdims=True) for h in hit], axis=0)
        pick_sum = jnp.sum(picked, axis=0, keepdims=True)
        gates = picked / pick_sum
        gate_ref[:, part] = gates
        scaled = loss_scale * gg[:, part]
        pick_grad = (scaled - jnp.sum(scaled * gates, axis=0, keepdims=True)) / pick_sum
        prob_grad = jnp.zeros_like(p)
        for j in range(top_k):
            prob_grad = jnp.where(hit[j], pick_grad[j:j + 1, :], prob_grad)
        prob_grad = prob_grad + f_bcast[...]
        grad = p * (prob_grad - jnp.sum(p * prob_grad, axis=0, keepdims=True))
        gt_ref[:, part] = grad.astype(jnp.bfloat16)

    small[0].wait()
    count_acc[...] = jnp.zeros_like(count_acc)
    prob_acc[...] = jnp.zeros_like(prob_acc)
    small[1].wait()
    tiles = rows // LANES
    first = 4

    @pl.loop(0, first)
    def _(b):
        logits(b)
        for u in range(tiles // first):
            count_tile(b * (tiles // first) + u)

    def exchange(buf, send, recv):
        return [remote(buf.at[me], buf.at[me], send.at[k], recv.at[k], at(k)) for k in range(1, 8)]

    cnt[me] = jnp.broadcast_to(jnp.sum(count_acc[...].T, axis=0, keepdims=True), (8, LANES))
    pl.semaphore_wait(barrier, 7)
    cnt_copies = exchange(cnt, cnt_send, cnt_recv)
    for c in cnt_copies:
        c.start()

    @pl.loop(first, blocks // 2)
    def _(b):
        logits(b)

    for c in cnt_copies:
        c.wait()
    freq = jnp.sum(cnt[...], axis=0) * (1.0 / total_rows)
    f_bcast[...] = jnp.broadcast_to(aux_coef * freq[:1, :], (experts, LANES)).T
    small[2].wait()

    @pl.loop(blocks // 2, blocks - 1)
    def _(b):
        logits(b)
        for u in range(4):
            backward_tile((b - blocks // 2) * 4 + u)

    logits(blocks - 1)
    for u in range(4):
        backward_tile(tiles - 4 + u)

    prob[me] = jnp.broadcast_to(jnp.sum(prob_acc[...].T, axis=0, keepdims=True), (8, LANES))
    prob_copies = exchange(prob, prob_send, prob_recv)

    def chip_at(flip):
        return at(2 * flip) // 2

    def columns(s):
        return pl.ds(pl.multiple_of(s * shard, shard), shard)

    def part_copy(i):
        return remote(send_part.at[i], from_part.at[i], part_send.at[i], part_recv.at[i], at(1))

    low, high = pl.ds(0, half), pl.ds(half, half)

    def x_copy(i, src):
        return remote(src, from_x.at[i], x_send.at[i], x_recv.at[i], at(2))

    def y_copy(i, src):
        return remote(src, from_y.at[i], y_send.at[i], y_recv.at[i], at(4))

    def combine(i):
        part_copy(i).wait_recv()
        own[i] = own[i] + from_part[i]

    y, x = chip // 2, chip % 2

    @pl.loop(0, 4)
    def _(i):
        flip = 3 - i
        fy, fx = flip // 2, flip % 2
        target = (y + fy) % 2 * 2 + (x + fx) % 2
        send_part[i] = jnp.dot(gt_ref[...], hid[:, columns(target * 2 + (1 - core))], preferred_element_type=jnp.float32)
        part_copy(i).start()

        @pl.when(i == 1)
        def _():
            combine(0)
            x_copy(0, own.at[0, low]).start()
            y_copy(0, own.at[0, high]).start()

        @pl.when(i == 2)
        def _():
            combine(1)
            y_copy(1, own.at[1, high]).start()

        @pl.when(i == 3)
        def _():
            combine(2)
            x_copy(1, own.at[2, low]).start()

        own[i] = jnp.dot(gt_ref[...], hid[:, columns(target * 2 + core)], preferred_element_type=jnp.float32)

    for c in prob_copies:
        c.start()

    x_copy(0, own.at[0, low]).wait_recv()
    own[1, low] = own[1, low] + from_x[0]
    y_copy(2, own.at[1, low]).start()
    y_copy(0, own.at[0, high]).wait_recv()
    own[2, high] = own[2, high] + from_y[0]
    x_copy(2, own.at[2, high]).start()

    combine(3)
    x_copy(1, own.at[2, low]).wait_recv()
    own[3, low] = own[3, low] + from_x[1]
    y_copy(1, own.at[1, high]).wait_recv()
    own[3, high] = own[3, high] + from_y[1]

    for c in prob_copies:
        c.wait()
    prob_mean = jnp.sum(prob[...], axis=0) * (1.0 / total_rows)
    freq_again = jnp.sum(cnt[...], axis=0) * (1.0 / total_rows)
    aux_ref[...] = jnp.broadcast_to(LOSS_ALPHA * experts * jnp.sum(freq_again * prob_mean, axis=1, keepdims=True), (8, LANES))

    y_copy(2, own.at[1, low]).wait_recv()
    own[3, low] = own[3, low] + from_y[2]
    x_copy(2, own.at[2, high]).wait_recv()
    own[3, high] = own[3, high] + from_x[2]
    gather[me] = own[3].T

    mine, xs, ys, ds = me, at(2), at(4), at(6)
    top, bottom = pl.ds(0, shard // 2), pl.ds(shard // 2, shard // 2)

    def gat_copy(k, src, device):
        return remote(src, src, gat_send.at[k], gat_recv.at[k], device)

    def out_copy(k, s):
        return pltpu.make_async_copy(gather.at[s], rg_hbm.at[pl.ds(pl.multiple_of(s * shard, shard), shard)], out_sem.at[k])

    to_x = gat_copy(0, gather.at[mine], at(2))
    to_y = gat_copy(1, gather.at[mine], at(4))
    to_p = gat_copy(4, gather.at[mine], at(1))
    to_x.start()
    to_y.start()
    to_p.start()
    out_copy(0, mine).start()
    to_x.wait_recv()
    fwd_y = gat_copy(2, gather.at[xs, top], at(4))
    fwd_y.start()
    part_x = gat_copy(5, gather.at[xs], at(1))
    part_x.start()
    out_copy(1, xs).start()
    to_y.wait_recv()
    fwd_x = gat_copy(3, gather.at[ys, bottom], at(2))
    fwd_x.start()
    part_y = gat_copy(6, gather.at[ys], at(1))
    part_y.start()
    out_copy(2, ys).start()
    fwd_y.wait_recv()
    fwd_x.wait_recv()
    part_d = gat_copy(7, gather.at[ds], at(1))
    part_d.start()
    out_copy(3, ds).start()
    to_p.wait_recv()
    out_copy(4, at(1)).start()
    part_x.wait_recv()
    out_copy(5, at(3)).start()
    part_y.wait_recv()
    out_copy(6, at(5)).start()
    part_d.wait_recv()
    out_copy(7, at(7)).start()

    @pl.loop(0, 4)
    def _(i):
        part_copy(i).wait_send()

    for i, src in enumerate((own.at[0, low], own.at[2, low], own.at[2, high])):
        x_copy(i, src).wait_send()
    for i, src in enumerate((own.at[0, high], own.at[1, high], own.at[1, low])):
        y_copy(i, src).wait_send()
    for c in (to_x, to_y, fwd_y, fwd_x, to_p, part_x, part_y, part_d):
        c.wait_send()
    for k, s in enumerate((mine, xs, ys, ds, at(1), at(3), at(5), at(7))):
        out_copy(k, s).wait()


def grad_kernel(gt_ref, w_ref, gate_in, aux_in, rg_in, hg_ref, gate_ref, aux_ref, rg_ref):
    out = lax.dot_general(gt_ref[...], w_ref[...], (((0,), (1,)), ((), ())), preferred_element_type=jnp.float32)
    hg_ref[...] = out.astype(jnp.bfloat16)
    gate_ref[...] = gate_in[...]
    aux_ref[...] = aux_in[...]
    rg_ref[...] = rg_in[...]


def solution(mesh):
    group_size = mesh.shape["dp"]

    def device_step(hidden, router_w, expert_idx, gate_grad):
        rows, width = hidden.shape
        experts, top_k = router_w.shape[1], expert_idx.shape[1]
        shard = width // 8
        f32, bf16 = jnp.float32, jnp.bfloat16
        any_spec, vmem_spec = pl.BlockSpec(memory_space=pl.ANY), pl.BlockSpec(memory_space=pltpu.VMEM)
        dma, vmem = pltpu.SemaphoreType.DMA, pltpu.VMEM

        def body(*refs):
            router_kernel(rows * group_size, *refs)

        gates, aux, gt, rg = pl.pallas_call(
            body,
            out_shape=(jax.ShapeDtypeStruct((top_k, rows), f32), jax.ShapeDtypeStruct((8, LANES), f32), jax.ShapeDtypeStruct((experts, rows), bf16), jax.ShapeDtypeStruct((width, experts), f32)),
            in_specs=[any_spec] * 4,
            out_specs=(vmem_spec, vmem_spec, vmem_spec, any_spec),
            scratch_shapes=[
                vmem((rows, width), bf16), vmem((width, experts), bf16), vmem((top_k, rows), jnp.int32), vmem((top_k, rows), f32),
                vmem((experts, rows), f32), vmem((experts, LANES), f32), vmem((experts, LANES), f32), vmem((experts, LANES), f32),
                vmem((8, 8, LANES), f32), vmem((8, 8, LANES), f32),
                vmem((4, experts, shard), f32), vmem((4, experts, shard), f32), vmem((4, experts, shard), f32),
                vmem((3, experts // 2, shard), f32), vmem((3, experts // 2, shard), f32), vmem((8, shard, experts), f32),
                dma((rows // 256,)), dma((3,)), dma((8,)), dma((8,)), dma((8,)), dma((8,)), dma((4,)), dma((4,)),
                dma((3,)), dma((3,)), dma((3,)), dma((3,)), dma((8,)), dma((8,)), dma((8,)),
            ],
            compiler_params=pltpu.CompilerParams(collective_id=0, has_side_effects=True, vmem_limit_bytes=56 * 2**20),
            name="router",
        )(hidden, router_w, expert_idx.T, gate_grad.T)

        steps = 16
        block, part = rows // steps, width // steps
        hidden_grad, gates, aux, rg = pl.pallas_call(
            grad_kernel,
            grid=(steps,),
            out_shape=(jax.ShapeDtypeStruct((rows, width), bf16), jax.ShapeDtypeStruct((top_k, rows), f32), jax.ShapeDtypeStruct((8, LANES), f32), jax.ShapeDtypeStruct((width, experts), f32)),
            in_specs=[
                pl.BlockSpec((experts, block), lambda i: (0, i)), pl.BlockSpec((width, experts), lambda i: (0, 0)), pl.BlockSpec((top_k, block), lambda i: (0, i)),
                pl.BlockSpec((8, LANES), lambda i: (0, 0)), pl.BlockSpec((part, experts), lambda i: (i, 0)),
            ],
            out_specs=(pl.BlockSpec((block, width), lambda i: (i, 0)), pl.BlockSpec((top_k, block), lambda i: (0, i)), pl.BlockSpec((8, LANES), lambda i: (0, 0)), pl.BlockSpec((part, experts), lambda i: (i, 0))),
            compiler_params=pltpu.CompilerParams(vmem_limit_bytes=40 * 2**20),
            name="hidden_grad",
        )(gt, router_w, gates, aux, rg)
        return gates.T, aux[0, 0], hidden_grad, rg

    return jax.shard_map(device_step, mesh=mesh, in_specs=(P("dp", None), P(None, None), P("dp", None), P("dp", None)), out_specs=(P("dp", None), P(), P("dp", None), P(None, None)), check_vma=False)
```
